32 devices in a mesh: dp: 2 (over x), tp: 16 (over y, z, core).
Axes of the slice: x: 2, y: 2, z: 4, core: 2. Of those that a mesh axis runs over, the one named last changes fastest.
Arguments:
- x: bfloat16 [4096, 4096], P('dp'), parts along dimension 0
- dy: bfloat16 [4096, 4096], P('dp'), parts along dimension 0
- gate: bfloat16 [4096, 16384], P('dp', 'tp'), parts along dimension 0
- up: bfloat16 [4096, 16384], P('dp', 'tp'), parts along dimension 0
- w_gate: bfloat16 [4096, 16384], P(None, 'tp')
- w_up: bfloat16 [4096, 16384], P(None, 'tp')
- w_down: bfloat16 [16384, 4096], P('tp')
Outputs:
- output 1: bfloat16 [4096, 4096], P('dp'), parts along dimension 0
- output 2: bfloat16 [8192, 16384], P('dp', 'tp'), parts along dimension 0
- output 3: bfloat16 [8192, 16384], P('dp', 'tp'), parts along dimension 0
- output 4: bfloat16 [32768, 4096], P(('dp', 'tp')), parts along dimension 0
There are 2 independent parts. The reference program is written for one: setup_inputs(seed, part) draws one part's arguments, and reference() takes and returns one part's arrays. A program takes and returns all parts, laid end to end along the dimension named above; an argument that names none is the same for every part.
All inputs are finite; a program needn't handle non-finite values.
Results may differ from the reference program's by a relative error of at most 0.012.
Values are sent between devices in bfloat16 or wider.
A program may use at most 2 GiB of HBM per device.

```python
import jax
import jax.numpy as jnp

ROWS = 2048
D = 4096
FF = 16384


def act(gate, up):
    return jax.nn.silu(gate) * up


def setup_inputs(seed: int = 0, part: int = 0) -> dict:
    kx, ky, ka, kb, kg, ku, kd = jax.random.split(jax.random.key(seed), 7)
    kx, ky, ka, kb = (jax.random.fold_in(k, part) for k in (kx, ky, ka, kb))
    drawn = {
        "x": jax.random.normal(kx, (ROWS, D), jnp.float32),
        "dy": jax.random.normal(ky, (ROWS, D), jnp.float32),
        "gate": jax.random.normal(ka, (ROWS, FF), jnp.float32),
        "up": jax.random.normal(kb, (ROWS, FF), jnp.float32),
        "w_gate": jax.random.normal(kg, (D, FF), jnp.float32) * D**-0.5,
        "w_up": jax.random.normal(ku, (D, FF), jnp.float32) * D**-0.5,
        "w_down": jax.random.normal(kd, (FF, D), jnp.float32) * FF**-0.5,
    }
    return {k: v.astype(jnp.bfloat16) for k, v in drawn.items()}


def reference(x, dy, gate, up, w_gate, w_up, w_down):
    hidden, back = jax.vjp(act, gate.astype(jnp.float32), up.astype(jnp.float32))
    d_hidden = jnp.dot(dy, w_down.T, preferred_element_type=jnp.float32)
    d_gate, d_up = (g.astype(jnp.bfloat16) for g in back(d_hidden))
    dx = jnp.dot(d_gate, w_gate.T, preferred_element_type=jnp.float32) + jnp.dot(d_up, w_up.T, preferred_element_type=jnp.float32)
    dw_gate = jnp.dot(x.T, d_gate, preferred_element_type=jnp.float32)
    dw_up = jnp.dot(x.T, d_up, preferred_element_type=jnp.float32)
    dw_down = jnp.dot(hidden.astype(jnp.bfloat16).T, dy, preferred_element_type=jnp.float32)
    return tuple(g.astype(jnp.bfloat16) for g in (dx, dw_gate, dw_up, dw_down))
```

```python
import functools

import jax
import jax.numpy as jnp
from jax import lax
from jax.experimental import pallas as pl
from jax.experimental.pallas import tpu as pltpu
from jax.sharding import PartitionSpec as P


F32, BF16 = jnp.float32, jnp.bfloat16
NT = (((1,), (1,)), ((), ()))
TN = (((0,), (0,)), ((), ()))
N = 8
CB = 256


def params(mib):
    return pltpu.CompilerParams(vmem_limit_bytes=mib << 20)


def in_hbm(v):
    return pltpu.with_memory_space_constraint(v, pltpu.HBM)


def cost(flops, bytes_accessed):
    return pl.CostEstimate(flops=flops, bytes_accessed=bytes_accessed, transcendentals=0)


def back_kernel(dy, w_down, gate, up, d_gate, d_up, hidden):
    d_hidden = lax.dot_general(dy[...], w_down[...], NT, preferred_element_type=F32)
    g, u = gate[...].astype(F32), up[...].astype(F32)
    s = jax.nn.sigmoid(g)
    a = g * s
    hidden[...] = (a * u).astype(BF16)
    d_up[...] = (d_hidden * a).astype(BF16)
    d_gate[...] = (d_hidden * u * (s + a * (1.0 - s))).astype(BF16)


def back(dy, w_down, gate, up, tile=1024, tf=256):
    (rows, d), f = dy.shape, gate.shape[1]
    wide = pl.BlockSpec((tile, tf), lambda i, j: (i, j))
    return pl.pallas_call(
        back_kernel,
        grid=(rows // tile, f // tf),
        in_specs=[pl.BlockSpec((tile, d), lambda i, j: (i, 0)), pl.BlockSpec((tf, d), lambda i, j: (j, 0)), wide, wide],
        out_specs=[wide] * 3,
        out_shape=[jax.ShapeDtypeStruct(gate.shape, BF16)] * 3,
        compiler_params=params(30),
        cost_estimate=cost(2 * rows * d * f, 2 * (rows * d + d * f + 5 * rows * f)),
    )(dy, w_down, gate, up)


ANY = pl.BlockSpec(memory_space=pl.ANY)


def column(place, offset, core):
    return lax.rem(place[0] + (offset + N), N) * 2 + core


def pick(offsets, k):
    o = offsets[-1]
    for i in range(len(offsets) - 1):
        o = jnp.where(k == i, offsets[i], o)
    return o


def term_kernel(place, dg, du, wg, wu, *rest):
    out = rest[-1]
    part = 1024

    @pl.loop(0, out.shape[0] // part)
    def _(i):
        r = pl.ds(pl.multiple_of(i * part, part), part)
        t = lax.dot_general(dg[r, :], wg[...], NT, preferred_element_type=F32)
        t = t + lax.dot_general(du[r, :], wu[...], NT, preferred_element_type=F32)
        out[r, :] = t.astype(out.dtype)


def terms(mine, place, offsets, dg, du, wg, wu, after=()):
    nb = len(offsets)
    rows, f = dg.shape
    lhs = pl.BlockSpec((rows, f), lambda j, p: (0, 0), pipeline_mode=pl.Buffered(1))
    rhs = pl.BlockSpec((CB, f), lambda j, p: (column(p, pick(offsets, j), p[1] if mine else 1 - p[1]), 0))
    return pl.pallas_call(
        term_kernel,
        grid_spec=pltpu.PrefetchScalarGridSpec(
            num_scalar_prefetch=1,
            grid=(nb,),
            in_specs=[lhs, lhs, rhs, rhs] + [ANY] * len(after),
            out_specs=pl.BlockSpec((rows, CB), lambda j, p: (0, j)),
        ),
        out_shape=jax.ShapeDtypeStruct((rows, nb * CB), F32 if mine else BF16),
        compiler_params=params(20),
        cost_estimate=cost(4 * nb * rows * CB * f, 4 * (rows + nb * CB) * f + 4 * rows * nb * CB),
    )(place, dg, du, wg, wu, *after)


def add_kernel(only, place, *refs):
    out = refs[-1]
    total = refs[0][...] + refs[1][...].astype(F32)
    for r in refs[2:-1]:
        v = r[...].astype(F32)
        total = total + (v if only is None else jnp.where(place[1] == only, v, jnp.zeros_like(v)))
    out[...] = total.astype(BF16)


def add(place, own, other, k, *got, only=None, tile=512):
    rows = own.shape[0]
    strip = pl.BlockSpec((tile, CB), lambda i, p: (i, k))
    piece = pl.BlockSpec((tile, CB), lambda i, p: (i, 0))
    return pl.pallas_call(
        functools.partial(add_kernel, only),
        grid_spec=pltpu.PrefetchScalarGridSpec(
            num_scalar_prefetch=1, grid=(rows // tile,), in_specs=[strip, strip] + [piece] * len(got), out_specs=piece
        ),
        out_shape=jax.ShapeDtypeStruct((rows, CB), BF16),
        compiler_params=params(8),
        cost_estimate=cost(2 * rows * CB, (8 + 2 * len(got)) * rows * CB),
    )(place, own, other, *got)


class Placing:
    def __init__(self, pieces, where):
        self.pieces, self.where = list(pieces), list(where)
        self.n = len(self.pieces)
        rows = self.pieces[0].shape[0] if self.n else 0
        self.scratch = (
            [pltpu.VMEM((self.n, rows, CB), BF16), pltpu.SemaphoreType.DMA((self.n,)), pltpu.SemaphoreType.DMA((self.n,))]
            if self.n
            else []
        )

    def run(self, step, steps, place, pieces, out, held, load, store):
        loads = [pltpu.make_async_copy(pieces[i], held.at[i], load.at[i]) for i in range(self.n)]
        stores = []
        for i, (o, mine) in enumerate(self.where):
            c = column(place, o, place[1] if mine else 1 - place[1])
            to = out.at[:, pl.ds(pl.multiple_of(c * CB, CB), CB)]
            stores.append(pltpu.make_async_copy(held.at[i], to, store.at[i]))

        @pl.when(step == 0)
        def _():
            for c in loads:
                c.start()

        @pl.when(step == min(1, steps - 1))
        def _():
            for a, b in zip(loads, stores):
                a.wait()
                b.start()

        @pl.when(step == steps - 1)
        def _():
            for c in stores:
                c.wait()


def weights_kernel(kind, steps, extra, placing, place, *refs):
    n = placing.n
    a = refs[: 3 if kind == "pair" else 2]
    pieces = refs[len(a) : len(a) + n]
    outs = refs[len(a) + n + extra :]
    step = pl.program_id(0)
    if n:
        placing.run(step, steps, place, pieces, outs[-4], *outs[-3:])
    if kind == "pair":
        x, dg, du = a
        outs[0][...] = lax.dot_general(x[...], dg[...], TN, preferred_element_type=F32).astype(BF16)
        outs[1][...] = lax.dot_general(x[...], du[...], TN, preferred_element_type=F32).astype(BF16)
    elif kind == "down":
        h, dy = a
        part = 512

        @pl.loop(0, h.shape[1] // part)
        def _(i):
            r = pl.ds(pl.multiple_of(i * part, part), part)
            outs[0][r, :] = lax.dot_general(h[:, r], dy[...], TN, preferred_element_type=F32).astype(BF16)


def weights(kind, place, a, first, count, before=(), dx=None, pieces=(), where=(), after=()):
    placing = Placing(pieces, where)
    tm = 512
    rows, f = a[1].shape if kind == "pair" else a[0].shape
    d = a[0].shape[1] if kind == "pair" else a[1].shape[1]
    whole = pl.BlockSpec((rows, f), lambda i, p: (0, 0), pipeline_mode=pl.Buffered(1))
    tile = pl.BlockSpec((rows, tm), lambda i, p: (0, first + i))
    if kind == "pair":
        ins, outs = [tile, whole, whole], [pl.BlockSpec((tm, f), lambda i, p: (first + i, 0))] * 2
        shapes = [jax.ShapeDtypeStruct((d, f), BF16)] * 2
    else:
        ins, outs = [whole, tile], [pl.BlockSpec((f, tm), lambda i, p: (0, first + i))]
        shapes = [jax.ShapeDtypeStruct((f, d), BF16)]
    given, after = [in_hbm(v) for v in before], [in_hbm(v) for v in after]
    if placing.n:
        given += [] if dx is None else [in_hbm(dx)]
        outs, shapes = outs + [ANY], shapes + [jax.ShapeDtypeStruct((rows, d), BF16)]
    at = 1 + len(ins) + placing.n
    alias = {at + i: i for i in range(len(before))}
    if placing.n and dx is not None:
        alias[at + len(before)] = len(shapes) - 1
    return pl.pallas_call(
        functools.partial(weights_kernel, kind, count, len(given) + len(after), placing),
        grid_spec=pltpu.PrefetchScalarGridSpec(
            num_scalar_prefetch=1,
            grid=(count,),
            in_specs=ins + [ANY] * (placing.n + len(given) + len(after)),
            out_specs=outs,
            scratch_shapes=placing.scratch,
        ),
        out_shape=shapes,
        input_output_aliases=alias,
        compiler_params=params((23 if kind == "pair" else 14) + placing.n),
        cost_estimate=cost(
            len(shapes[: 2 if kind == "pair" else 1]) * 2 * rows * tm * count * f,
            2 * (rows * tm * count + 2 * rows * f + 2 * tm * count * f),
        ),
    )(place, *a, *pieces, *given, *after)


def place_kernel(placing, extra, place, *refs):
    outs = refs[placing.n + extra :]
    placing.run(jnp.int32(0), 1, place, refs[: placing.n], outs[0], *outs[1:])


def put(place, dx, pieces, where):
    placing = Placing(pieces, where)
    n = placing.n
    return pl.pallas_call(
        functools.partial(place_kernel, placing, 1),
        grid_spec=pltpu.PrefetchScalarGridSpec(
            num_scalar_prefetch=1, grid=(), in_specs=[ANY] * (n + 1), out_specs=ANY, scratch_shapes=placing.scratch
        ),
        out_shape=jax.ShapeDtypeStruct(dx.shape, BF16),
        input_output_aliases={1 + n: 0},
        compiler_params=params(14),
        cost_estimate=cost(n * dx.shape[0] * CB, 4 * n * dx.shape[0] * CB),
    )(place, *pieces, dx)


def ring_order():
    def chip(p):
        p %= N
        return p if p < 4 else 4 + (N - 1 - p)

    return lambda p, c: chip(p) * 2 + c


def solution(mesh):
    dev = ring_order()
    right = [(dev(p, c), dev(p + 1, c)) for p in range(N) for c in (0, 1)]
    left = [(dev(p, c), dev(p - 1, c)) for p in range(N) for c in (0, 1)]
    apart = [(dev(p, c), dev(p + 1 - 2 * c, c)) for p in range(N) for c in (0, 1)]
    swap = [(dev(p, c), dev(p, 1 - c)) for p in range(N) for c in (0, 1)]

    def send(v, pairs):
        return lax.ppermute(v, "tp", pairs)

    def step(x, dy, gate, up, w_gate, w_up, w_down):
        index = lax.axis_index("tp")
        core, chip = index % 2, index // 2
        place = jnp.stack([jnp.where(chip < 4, chip, N + 3 - chip), core]).astype(jnp.int32)
        x, dy, gate, up, w_gate, w_up, w_down = (
            in_hbm(v) for v in (x, dy, gate, up, w_gate, w_up, w_down)
        )
        d_gate, d_up, hidden = back(dy, w_down, gate, up)
        hidden = in_hbm(hidden)
        d_gate, d_up = (pltpu.with_memory_space_constraint(v, pltpu.VMEM) for v in (d_gate, d_up))

        def stage(o, *after):
            given = (place, o, d_gate, d_up, w_gate, w_up, after)
            other = terms(False, *given)
            other = send(other, swap)
            return other, terms(True, *given)

        def gradients(kind, first, count, *more):
            given = (hidden, dy) if kind == "down" else (x, d_gate, d_up)
            return weights(kind, place, given, first, count, *more)

        def both(v):
            return [(-v, True), (v, True)], [(-v, False), (v, False)]

        other, own = stage((4,))
        far = add(place, own, other, 0)
        other, own = stage((3, -3), far)
        dw_down = ()
        got_r = got_l = send(far, apart)
        for o, then in ((3, (2, -2)), (2, (1, -1)), (1, (0,))):
            to_r = add(place, own, other, 0, got_r, only=0 if o == 3 else None)
            to_l = add(place, own, other, 1, got_l, only=1 if o == 3 else None)
            other, own = stage(then, to_r, to_l)
            got_r, got_l = send(to_r, right), send(to_l, left)
            first, count = {3: (0, 1), 2: (1, 1), 1: (2, 2)}[o]
            dw_down = gradients("down", first, count, dw_down)
        done = add(place, own, other, 0, got_r, got_l)

        a1 = [send(done, right), send(done, left)]
        b0 = [send(done, swap)]
        *dw, dx = gradients("pair", 0, 3, (), None, [done], [(0, True)])
        a2 = [send(a1[0], right), send(a1[1], left)]
        b1 = [send(v, swap) for v in a1]
        *dw, dx = gradients("pair", 3, 3, dw, dx, b0 + a1, [(0, False)] + both(1)[0])
        a3 = [send(a2[0], right), send(a2[1], left)]
        b2 = [send(v, swap) for v in a2]
        *dw, dx = gradients("pair", 6, 2, dw, dx, b1 + a2, both(1)[1] + both(2)[0])
        dw_down = gradients("down", 4, 1, dw_down, None, (), (), (dx,))
        last = send(jnp.where(core == 0, a3[0], a3[1]), apart)
        b3 = [send(v, swap) for v in a3]
        dw_down, dx = gradients("down", 5, 3, dw_down, dx, b2 + a3, both(2)[1] + both(3)[0])
        dx = put(place, dx, b3, both(3)[1])
        dx = put(place, dx, [last, send(last, swap)], [(4, True), (4, False)])
        return dx, *dw, dw_down

    tokens, columns, rows = P("dp", None), P(None, "tp"), P("tp", None)
    return jax.shard_map(
        step,
        mesh=mesh,
        in_specs=(tokens, tokens, P("dp", "tp"), P("dp", "tp"), columns, columns, rows),
        out_specs=(tokens, P("dp", "tp"), P("dp", "tp"), P(("dp", "tp"), None)),
        check_vma=False,
    )
```

```python
import functools

import jax
import jax.numpy as jnp
from jax import lax
from jax.experimental import pallas as pl
from jax.experimental.pallas import tpu as pltpu
from jax.sharding import PartitionSpec as P


F32, BF16 = jnp.float32, jnp.bfloat16
NT = (((1,), (1,)), ((), ()))
TN = (((0,), (0,)), ((), ()))
N = 8
CB = 256


def params(mib):
    return pltpu.CompilerParams(vmem_limit_bytes=mib << 20)


def in_hbm(v):
    return pltpu.with_memory_space_constraint(v, pltpu.HBM)


def cost(flops, bytes_accessed):
    return pl.CostEstimate(flops=flops, bytes_accessed=bytes_accessed, transcendentals=0)


def back_kernel(dy, w_down, gate, up, d_gate, d_up, hidden):
    d_hidden = lax.dot_general(dy[...], w_down[...], NT, preferred_element_type=F32)
    g, u = gate[...].astype(F32), up[...].astype(F32)
    s = jax.nn.sigmoid(g)
    a = g * s
    hidden[...] = (a * u).astype(BF16)
    d_up[...] = (d_hidden * a).astype(BF16)
    d_gate[...] = (d_hidden * u * (s + a * (1.0 - s))).astype(BF16)


def back(dy, w_down, gate, up, tile=1024, tf=256):
    (rows, d), f = dy.shape, gate.shape[1]
    wide = pl.BlockSpec((tile, tf), lambda i, j: (i, j))
    return pl.pallas_call(
        back_kernel,
        grid=(rows // tile, f // tf),
        in_specs=[pl.BlockSpec((tile, d), lambda i, j: (i, 0)), pl.BlockSpec((tf, d), lambda i, j: (j, 0)), wide, wide],
        out_specs=[wide] * 3,
        out_shape=[jax.ShapeDtypeStruct(gate.shape, BF16)] * 3,
        compiler_params=params(30),
        cost_estimate=cost(2 * rows * d * f, 2 * (rows * d + d * f + 5 * rows * f)),
    )(dy, w_down, gate, up)


ANY = pl.BlockSpec(memory_space=pl.ANY)


def column(place, offset, core):
    return lax.rem(place[0] + (offset + N), N) * 2 + core


def pick(offsets, k):
    o = offsets[-1]
    for i in range(len(offsets) - 1):
        o = jnp.where(k == i, offsets[i], o)
    return o


def term_kernel(place, dg, du, wg, wu, *rest):
    out = rest[-1]
    part = 1024

    @pl.loop(0, out.shape[0] // part)
    def _(i):
        r = pl.ds(pl.multiple_of(i * part, part), part)
        t = lax.dot_general(dg[r, :], wg[...], NT, preferred_element_type=F32)
        t = t + lax.dot_general(du[r, :], wu[...], NT, preferred_element_type=F32)
        out[r, :] = t.astype(out.dtype)


def terms(mine, place, offsets, dg, du, wg, wu, after=()):
    nb = len(offsets)
    rows, f = dg.shape
    lhs = pl.BlockSpec((rows, f), lambda j, p: (0, 0), pipeline_mode=pl.Buffered(1))
    rhs = pl.BlockSpec((CB, f), lambda j, p: (column(p, pick(offsets, j), p[1] if mine else 1 - p[1]), 0))
    return pl.pallas_call(
        term_kernel,
        grid_spec=pltpu.PrefetchScalarGridSpec(
            num_scalar_prefetch=1,
            grid=(nb,),
            in_specs=[lhs, lhs, rhs, rhs] + [ANY] * len(after),
            out_specs=pl.BlockSpec((rows, CB), lambda j, p: (0, j)),
        ),
        out_shape=jax.ShapeDtypeStruct((rows, nb * CB), F32 if mine else BF16),
        compiler_params=params(20),
        cost_estimate=cost(4 * nb * rows * CB * f, 4 * (rows + nb * CB) * f + 4 * rows * nb * CB),
    )(place, dg, du, wg, wu, *after)


def both_kernel(nb, place, dg, du, wg, wu, *rest):
    other, own = rest[-2:]
    part = 1024

    @pl.loop(0, own.shape[0] // part)
    def _(i):
        r = pl.ds(pl.multiple_of(i * part, part), part)
        t = lax.dot_general(dg[r, :], wg[...], NT, preferred_element_type=F32)
        t = t + lax.dot_general(du[r, :], wu[...], NT, preferred_element_type=F32)

        @pl.when(pl.program_id(0) < nb)
        def _():
            other[r, :] = t.astype(BF16)

        @pl.when(pl.program_id(0) >= nb)
        def _():
            own[r, :] = t


def both_terms(place, offsets, dg, du, wg, wu, after=()):
    nb = len(offsets)
    rows, f = dg.shape
    lhs = pl.BlockSpec((rows, f), lambda j, p: (0, 0), pipeline_mode=pl.Buffered(1))
    rhs = pl.BlockSpec(
        (CB, f), lambda j, p: (column(p, pick(offsets, lax.rem(j, nb)), jnp.where(j < nb, 1 - p[1], p[1])), 0)
    )
    return pl.pallas_call(
        functools.partial(both_kernel, nb),
        grid_spec=pltpu.PrefetchScalarGridSpec(
            num_scalar_prefetch=1,
            grid=(2 * nb,),
            in_specs=[lhs, lhs, rhs, rhs] + [ANY] * len(after),
            out_specs=[
                pl.BlockSpec((rows, CB), lambda j, p: (0, jnp.minimum(j, nb - 1))),
                pl.BlockSpec((rows, CB), lambda j, p: (0, jnp.maximum(j - nb, 0))),
            ],
        ),
        out_shape=[jax.ShapeDtypeStruct((rows, nb * CB), BF16), jax.ShapeDtypeStruct((rows, nb * CB), F32)],
        compiler_params=params(22),
        cost_estimate=cost(8 * nb * rows * CB * f, 4 * (rows + 2 * nb * CB) * f + 6 * rows * nb * CB),
    )(place, *(dg, du, wg, wu), *after)


def add_kernel(only, place, *refs):
    out = refs[-1]
    total = refs[0][...] + refs[1][...].astype(F32)
    for r in refs[2:-1]:
        v = r[...].astype(F32)
        total = total + (v if only is None else jnp.where(place[1] == only, v, jnp.zeros_like(v)))
    out[...] = total.astype(BF16)


def add(place, own, other, k, *got, only=None, tile=512):
    rows = own.shape[0]
    strip = pl.BlockSpec((tile, CB), lambda i, p: (i, k))
    piece = pl.BlockSpec((tile, CB), lambda i, p: (i, 0))
    return pl.pallas_call(
        functools.partial(add_kernel, only),
        grid_spec=pltpu.PrefetchScalarGridSpec(
            num_scalar_prefetch=1, grid=(rows // tile,), in_specs=[strip, strip] + [piece] * len(got), out_specs=piece
        ),
        out_shape=jax.ShapeDtypeStruct((rows, CB), BF16),
        compiler_params=params(8),
        cost_estimate=cost(2 * rows * CB, (8 + 2 * len(got)) * rows * CB),
    )(place, own, other, *got)


class Placing:
    def __init__(self, pieces, where):
        self.pieces, self.where = list(pieces), list(where)
        self.n = len(self.pieces)
        rows = self.pieces[0].shape[0] if self.n else 0
        self.scratch = (
            [pltpu.VMEM((self.n, rows, CB), BF16), pltpu.SemaphoreType.DMA((self.n,)), pltpu.SemaphoreType.DMA((self.n,))]
            if self.n
            else []
        )

    def run(self, step, steps, place, pieces, out, held, load, store):
        loads = [pltpu.make_async_copy(pieces[i], held.at[i], load.at[i]) for i in range(self.n)]
        stores = []
        for i, (o, mine) in enumerate(self.where):
            c = column(place, o, place[1] if mine else 1 - place[1])
            to = out.at[:, pl.ds(pl.multiple_of(c * CB, CB), CB)]
            stores.append(pltpu.make_async_copy(held.at[i], to, store.at[i]))

        @pl.when(step == 0)
        def _():
            for c in loads:
                c.start()

        @pl.when(step == min(1, steps - 1))
        def _():
            for a, b in zip(loads, stores):
                a.wait()
                b.start()

        @pl.when(step == steps - 1)
        def _():
            for c in stores:
                c.wait()


def weights_kernel(kind, steps, extra, placing, place, *refs):
    n = placing.n
    a = refs[: 3 if kind == "pair" else 2]
    pieces = refs[len(a) : len(a) + n]
    outs = refs[len(a) + n + extra :]
    step = pl.program_id(0)
    if n:
        placing.run(step, steps, place, pieces, outs[-4], *outs[-3:])
    if kind == "pair":
        x, dg, du = a
        outs[0][...] = lax.dot_general(x[...], dg[...], TN, preferred_element_type=F32).astype(BF16)
        outs[1][...] = lax.dot_general(x[...], du[...], TN, preferred_element_type=F32).astype(BF16)
    elif kind == "down":
        h, dy = a
        part = 512

        @pl.loop(0, h.shape[1] // part)
        def _(i):
            r = pl.ds(pl.multiple_of(i * part, part), part)
            outs[0][r, :] = lax.dot_general(h[:, r], dy[...], TN, preferred_element_type=F32).astype(BF16)


def weights(kind, place, a, first, count, before=(), dx=None, pieces=(), where=(), after=()):
    placing = Placing(pieces, where)
    tm = 512
    rows, f = a[1].shape if kind == "pair" else a[0].shape
    d = a[0].shape[1] if kind == "pair" else a[1].shape[1]
    whole = pl.BlockSpec((rows, f), lambda i, p: (0, 0), pipeline_mode=pl.Buffered(1))
    tile = pl.BlockSpec((rows, tm), lambda i, p: (0, first + i))
    if kind == "pair":
        ins, outs = [tile, whole, whole], [pl.BlockSpec((tm, f), lambda i, p: (first + i, 0))] * 2
        shapes = [jax.ShapeDtypeStruct((d, f), BF16)] * 2
    else:
        ins, outs = [whole, tile], [pl.BlockSpec((f, tm), lambda i, p: (0, first + i))]
        shapes = [jax.ShapeDtypeStruct((f, d), BF16)]
    given, after = [in_hbm(v) for v in before], [in_hbm(v) for v in after]
    if placing.n:
        given += [] if dx is None else [in_hbm(dx)]
        outs, shapes = outs + [ANY], shapes + [jax.ShapeDtypeStruct((rows, d), BF16)]
    at = 1 + len(ins) + placing.n
    alias = {at + i: i for i in range(len(before))}
    if placing.n and dx is not None:
        alias[at + len(before)] = len(shapes) - 1
    return pl.pallas_call(
        functools.partial(weights_kernel, kind, count, len(given) + len(after), placing),
        grid_spec=pltpu.PrefetchScalarGridSpec(
            num_scalar_prefetch=1,
            grid=(count,),
            in_specs=ins + [ANY] * (placing.n + len(given) + len(after)),
            out_specs=outs,
            scratch_shapes=placing.scratch,
        ),
        out_shape=shapes,
        input_output_aliases=alias,
        compiler_params=params((23 if kind == "pair" else 14) + placing.n),
        cost_estimate=cost(
            len(shapes[: 2 if kind == "pair" else 1]) * 2 * rows * tm * count * f,
            2 * (rows * tm * count + 2 * rows * f + 2 * tm * count * f),
        ),
    )(place, *a, *pieces, *given, *after)


def place_kernel(placing, extra, place, *refs):
    outs = refs[placing.n + extra :]
    placing.run(jnp.int32(0), 1, place, refs[: placing.n], outs[0], *outs[1:])


def put(place, dx, pieces, where):
    placing = Placing(pieces, where)
    n = placing.n
    return pl.pallas_call(
        functools.partial(place_kernel, placing, 1),
        grid_spec=pltpu.PrefetchScalarGridSpec(
            num_scalar_prefetch=1, grid=(), in_specs=[ANY] * (n + 1), out_specs=ANY, scratch_shapes=placing.scratch
        ),
        out_shape=jax.ShapeDtypeStruct(dx.shape, BF16),
        input_output_aliases={1 + n: 0},
        compiler_params=params(14),
        cost_estimate=cost(n * dx.shape[0] * CB, 4 * n * dx.shape[0] * CB),
    )(place, *pieces, dx)


def ring_order():
    def chip(p):
        p %= N
        return p if p < 4 else 4 + (N - 1 - p)

    return lambda p, c: chip(p) * 2 + c


def solution(mesh):
    dev = ring_order()
    right = [(dev(p, c), dev(p + 1, c)) for p in range(N) for c in (0, 1)]
    left = [(dev(p, c), dev(p - 1, c)) for p in range(N) for c in (0, 1)]
    apart = [(dev(p, c), dev(p + 1 - 2 * c, c)) for p in range(N) for c in (0, 1)]
    swap = [(dev(p, c), dev(p, 1 - c)) for p in range(N) for c in (0, 1)]

    def send(v, pairs):
        return lax.ppermute(v, "tp", pairs)

    def step(x, dy, gate, up, w_gate, w_up, w_down):
        index = lax.axis_index("tp")
        core, chip = index % 2, index // 2
        place = jnp.stack([jnp.where(chip < 4, chip, N + 3 - chip), core]).astype(jnp.int32)
        x, dy, gate, up, w_gate, w_up, w_down = (
            in_hbm(v) for v in (x, dy, gate, up, w_gate, w_up, w_down)
        )
        d_gate, d_up, hidden = back(dy, w_down, gate, up)
        hidden = in_hbm(hidden)
        d_gate, d_up = (pltpu.with_memory_space_constraint(v, pltpu.VMEM) for v in (d_gate, d_up))

        def stage(o, *after):
            given = (place, o, d_gate, d_up, w_gate, w_up, after)
            if o[0] < 3:
                other, own = both_terms(*given)
                return send(other, swap), own
            other = terms(False, *given)
            other = send(other, swap)
            return other, terms(True, *given)

        def gradients(kind, first, count, *more):
            given = (hidden, dy) if kind == "down" else (x, d_gate, d_up)
            return weights(kind, place, given, first, count, *more)

        def both(v):
            return [(-v, True), (v, True)], [(-v, False), (v, False)]

        other, own = stage((4,))
        far = add(place, own, other, 0)
        other, own = stage((3, -3), far)
        dw = ()
        got_r = got_l = send(far, apart)
        for o, then in ((3, (2, -2)), (2, (1, -1)), (1, (0,))):
            to_r = add(place, own, other, 0, got_r, only=0 if o == 3 else None)
            to_l = add(place, own, other, 1, got_l, only=1 if o == 3 else None)
            other, own = stage(then, to_r, to_l)
            got_r, got_l = send(to_r, right), send(to_l, left)
            if o != 2:
                first, count = {3: (0, 1), 1: (1, 3)}[o]
                dw = gradients("pair", first, count, dw)
        done = add(place, own, other, 0, got_r, got_l)

        a1 = [send(done, right), send(done, left)]
        b0 = [send(done, swap)]
        *dw, dx = gradients("pair", 4, 4, dw, None, [done], [(0, True)])
        a2 = [send(a1[0], right), send(a1[1], left)]
        b1 = [send(v, swap) for v in a1]
        dw_down, dx = gradients("down", 0, 5, (), dx, b0 + a1, [(0, False)] + both(1)[0])
        a3 = [send(a2[0], right), send(a2[1], left)]
        b2 = [send(v, swap) for v in a2]
        dw_down, dx = gradients("down", 5, 3, (dw_down,), dx, b1 + a2, both(1)[1] + both(2)[0])
        last = send(jnp.where(core == 0, a3[0], a3[1]), apart)
        b3 = [send(v, swap) for v in a3]
        dx = put(place, dx, b2 + a3, both(2)[1] + both(3)[0])
        dx = put(place, dx, b3, both(3)[1])
        dx = put(place, dx, [last, send(last, swap)], [(4, True), (4, False)])
        return dx, *dw, dw_down

    tokens, columns, rows = P("dp", None), P(None, "tp"), P("tp", None)
    return jax.shard_map(
        step,
        mesh=mesh,
        in_specs=(tokens, tokens, P("dp", "tp"), P("dp", "tp"), columns, columns, rows),
        out_specs=(tokens, P("dp", "tp"), P("dp", "tp"), P(("dp", "tp"), None)),
        check_vma=False,
    )
```
